32 devices in a mesh: gx: 2 (over x), gy: 4 (over y, core), gz: 4 (over z).
Axes of the slice: x: 2, y: 2, z: 4, core: 2. Of those that a mesh axis runs over, the one named last changes fastest.
Arguments:
- state: float32 [5, 12, 96, 1536], P(None, 'gx', 'gy', 'gz'), as said below
- register: float32 [5, 12, 96, 1536], P(None, 'gx', 'gy', 'gz'), may hold values from -0.25 to 0.25
Outputs:
- new_state: float32 [5, 12, 96, 1536], P(None, 'gx', 'gy', 'gz')
- new_register: float32 [5, 12, 96, 1536], P(None, 'gx', 'gy', 'gz')
The draws below stay inside these ranges and needn't reach their ends.
Inputs may be any that keep to these rules, and one draw needn't show every extreme that they name: Density is between 0.5 and 2.5, and the pressure computed from the state is positive.
All inputs are finite; a program needn't handle non-finite values.
Results may differ from the reference program's by a relative error of at most 0.0003.
Values sent between devices are 32-bit elements; how exact they have to be, the bound alone decides.
No kernel may reach another device: no remote copies, remote signals or barrier semaphores. Data moves between devices by JAX's collectives and lax.ppermute only.
A program may use at most 128 MiB of HBM per device.

```python
import math
import jax
import jax.numpy as jnp
import numpy as np
from jax import lax

NVAR = 5
NXN = 12
NYN = 96
NZN = 1536


def smooth_field(key, grid, amplitude):
    xpos = lax.broadcasted_iota(jnp.float32, grid, 0) / grid[0]
    ypos = lax.broadcasted_iota(jnp.float32, grid, 1) / grid[1]
    zpos = lax.broadcasted_iota(jnp.float32, grid, 2) / grid[2]
    waves = jax.random.randint(jax.random.fold_in(key, 1), (4, 3), 1, 4).astype(jnp.float32)
    phases = jax.random.uniform(jax.random.fold_in(key, 2), (4,), jnp.float32, 0.0, 6.283185307179586)
    total = jnp.zeros(grid, jnp.float32)
    for mode in range(4):
        angle = 6.283185307179586 * (waves[mode, 0] * xpos + waves[mode, 1] * ypos + waves[mode, 2] * zpos) + phases[mode]
        total = total + amplitude * jnp.sin(angle)
    return total


def draw_state(key, part):
    key_rho = jax.random.fold_in(key, 11)
    key_vel = jax.random.fold_in(key, 12)
    key_press = jax.random.fold_in(key, 13)
    grid = (NXN, NYN, NZN)
    xpos = lax.broadcasted_iota(jnp.float32, grid, 0) / NXN
    amp = 1.0 + 2.0 * xpos
    noise = 0.015 * jnp.clip(jax.random.normal(jax.random.fold_in(key_vel, 5), (3,) + grid, jnp.float32), -3.0, 3.0)
    rho_noise = 0.03 * jnp.clip(jax.random.normal(jax.random.fold_in(key_rho, 5), grid, jnp.float32), -3.0, 3.0)
    press_noise = 0.03 * jnp.clip(jax.random.normal(jax.random.fold_in(key_press, 5), grid, jnp.float32), -3.0, 3.0)
    density = 1.0 + smooth_field(key_rho, grid, 0.08) + rho_noise
    press = 1.0 + smooth_field(key_press, grid, 0.08) + press_noise
    vel = jnp.stack([amp * smooth_field(jax.random.fold_in(key_vel, c), grid, 0.1) for c in range(3)]) + noise
    energy = press / 0.4 + 0.5 * density * jnp.sum(vel * vel, axis=0)
    return jnp.concatenate([density[None], density[None] * vel, energy[None]], axis=0).astype(jnp.float32)


def block_scale(rng, extent, pieces, smallest, high):
    loudness = 1.0
    for axis_at, blocks in pieces:
        heights = jax.random.uniform(jax.random.fold_in(jax.random.fold_in(rng, 6), axis_at), (blocks,), jnp.float32, smallest / len(pieces), high / len(pieces))
        loudness = loudness * jnp.repeat(jnp.exp(heights), extent[axis_at] // blocks).reshape((-1,) + (1,) * (len(extent) - 1 - axis_at))
    return loudness


def centred(stream_key, shape, deviation, limit, cuts=(), dtype=jnp.bfloat16):
    result = deviation * jax.random.normal(stream_key, shape, jnp.float32)
    if cuts:
        result = result * block_scale(stream_key, shape, cuts, -0.22, 0.18)
    return jnp.clip(result, -limit, limit).astype(dtype)


def setup_inputs(seed: int = 0) -> dict:
    splits = jax.random.split(jax.random.key(seed), 3)
    state = draw_state(jax.random.fold_in(splits[2], 71), 0)
    register = centred(splits[1], (NVAR, NXN, NYN, NZN), 0.05, 0.25, ((1, 2), (2, 4), (3, 4)), jnp.float32)
    return dict(state=state, register=register)


GAMMA = 1.4
GM1 = 0.4
ELEM_WIDTH = 0.05
COURANT = 0.5
INV_W = 15.0
COEFFS = ((-567301805773.0 / 1357537059087.0, 5161836677717.0 / 13612068292357.0), (-2404267990393.0 / 2016746695238.0, 1720146321549.0 / 2090206949498.0))
FORMS = ('ij,vejyz->veiyz', 'ij,vxejz->vxeiz', 'ij,vxyej->vxyei')

def gll_derivative():
    seven = math.sqrt(7.0)
    inner = math.sqrt(1.0 / 3.0 - 2.0 * seven / 21.0)
    outer = math.sqrt(1.0 / 3.0 + 2.0 * seven / 21.0)
    points = np.array([-1.0, -outer, -inner, inner, outer, 1.0])
    count = len(points)
    weights = np.array([np.prod([points[i] - points[j] for j in range(count) if j != i]) for i in range(count)])
    table = np.zeros((count, count))
    for i in range(count):
        for j in range(count):
            if i != j:
                table[i, j] = weights[i] / weights[j] / (points[i] - points[j])
        table[i, i] = -np.sum(table[i])
    return table

def pressure(u):
    mom_sq = u[1] * u[1] + u[2] * u[2] + u[3] * u[3]
    return (GM1 * (u[4] - 0.5 * mom_sq / u[0]), mom_sq)

def euler_flux(u, d):
    press, mom_sq = pressure(u)
    vel = u[1 + d] / u[0]
    parts = [u[1 + d], u[1] * vel, u[2] * vel, u[3] * vel, (u[4] + press) * vel]
    parts[1 + d] = parts[1 + d] + press
    speed = jnp.abs(vel) + jnp.sqrt(GAMMA * press / u[0])
    return (jnp.stack(parts), speed)

def direction_term(ext, d, diff):
    axis = 1 + d
    nodes = diff.shape[0]
    full = ext.shape[axis]
    length = full - 2
    elems = length // nodes
    inner = lax.slice_in_dim(ext, 1, full - 1, axis=axis)
    flux_in, unused = euler_flux(inner, d)
    shape = flux_in.shape
    blocked = flux_in.reshape(shape[:axis] + (elems, nodes) + shape[axis + 1:])
    deriv = jnp.einsum(FORMS[d], diff, blocked, precision=lax.Precision.HIGHEST).reshape(shape)
    lower_side = lax.slice_in_dim(ext, 0, length + 1, nodes, axis)
    upper_side = lax.slice_in_dim(ext, 1, length + 2, nodes, axis)
    flux_low, speed_low = euler_flux(lower_side, d)
    flux_up, speed_up = euler_flux(upper_side, d)
    lam = jnp.maximum(speed_low, speed_up)
    fstar = 0.5 * (flux_low + flux_up) - 0.5 * lam[None] * (upper_side - lower_side)
    first = lax.slice_in_dim(flux_in, 0, length, nodes, axis)
    last = lax.slice_in_dim(flux_in, nodes - 1, length, nodes, axis)
    lower = -(first - lax.slice_in_dim(fstar, 0, elems, axis=axis)) * INV_W
    upper = (last - lax.slice_in_dim(fstar, 1, elems + 1, axis=axis)) * INV_W
    bshape = shape[:axis] + (elems, 1) + shape[axis + 1:]
    zeros = jnp.zeros(shape[:axis] + (elems, nodes - 2) + shape[axis + 1:], jnp.float32)
    corr = jnp.concatenate([lower.reshape(bshape), zeros, upper.reshape(bshape)], axis=axis + 1).reshape(shape)
    return 2.0 / ELEM_WIDTH * (corr - deriv)

def max_speed(u):
    press, mom_sq = pressure(u)
    return jnp.max(jnp.sqrt(mom_sq) / u[0] + jnp.sqrt(GAMMA * press / u[0]))

def residual_of(u, diff):
    total = jnp.zeros_like(u)
    for d in range(3):
        pads = [(0, 0)] * 4
        pads[1 + d] = (1, 1)
        ext = jnp.pad(u, pads, mode='wrap')
        total = total + direction_term(ext, d, diff)
    return total

def reference(state, register):
    diff = jnp.asarray(gll_derivative(), jnp.float32)
    step = COURANT * ELEM_WIDTH / (11.0 * max_speed(state))
    current = state
    section_reg = register
    for coef_a, coef_b in COEFFS:
        section_reg = coef_a * section_reg + step * residual_of(current, diff)
        current = current + coef_b * section_reg
    return (current, section_reg)
```

```python
import math

import jax
import jax.numpy as jnp
import numpy as np
from jax import lax
from jax.experimental import pallas as pl
from jax.experimental.pallas import tpu as pltpu
from jax.sharding import PartitionSpec as P

GAMMA = 1.4
GM1 = 0.4
ELEM_WIDTH = 0.05
COURANT = 0.5
INV_W = 15.0
NODES = 6
SCALE = 2.0 / ELEM_WIDTH
LIFT = 0.5 * SCALE * INV_W
COEFFS = (
    (-567301805773.0 / 1357537059087.0, 5161836677717.0 / 13612068292357.0),
    (-2404267990393.0 / 2016746695238.0, 1720146321549.0 / 2090206949498.0),
)
LANES = 128
ROWS = 8


def gll_derivative():
    seven = math.sqrt(7.0)
    inner = math.sqrt(1.0 / 3.0 - 2.0 * seven / 21.0)
    outer = math.sqrt(1.0 / 3.0 + 2.0 * seven / 21.0)
    points = np.array([-1.0, -outer, -inner, inner, outer, 1.0])
    count = len(points)
    weights = np.array(
        [np.prod([points[i] - points[j] for j in range(count) if j != i]) for i in range(count)]
    )
    table = np.zeros((count, count))
    for i in range(count):
        for j in range(count):
            if i != j:
                table[i, j] = weights[i] / weights[j] / (points[i] - points[j])
        table[i, i] = -np.sum(table[i])
    return table


def flux_matrix(length):
    table = np.kron(np.eye(length // NODES), -SCALE * gll_derivative())
    for up in range(NODES, length, NODES):
        low = up - 1
        table[low, low] += LIFT
        table[low, up] -= LIFT
        table[up, low] += LIFT
        table[up, up] -= LIFT
    return table


def split_bf16(table):
    table = np.asarray(table, np.float32)
    high = table.astype(jnp.bfloat16)
    low = (table - high.astype(np.float32)).astype(jnp.bfloat16)
    return jnp.asarray(high), jnp.asarray(low)


def face_masks(length):
    place = np.arange(length)
    last = (place % NODES == NODES - 1).astype(np.float32)
    ends = (place % NODES == 0) | (place % NODES == NODES - 1)
    ends = ends & (place != 0) & (place != length - 1)
    return last, LIFT * ends.astype(np.float32)


def primitives(u):
    inv = 1.0 / u[0]
    vel = [u[1] * inv, u[2] * inv, u[3] * inv]
    kinetic = u[1] * vel[0] + u[2] * vel[1] + u[3] * vel[2]
    press = GM1 * (u[4] - 0.5 * kinetic)
    return inv, vel, press


def flux(u, vel, press, d):
    v = vel[d]
    parts = [u[1 + d], u[1] * v, u[2] * v, u[3] * v, (u[4] + press) * v]
    parts[1 + d] = parts[1 + d] + press
    return parts


def face_lift(u, other, d, sign):
    inv, vel, press = primitives(u)
    inv_o, vel_o, press_o = primitives(other)
    mine = flux(u, vel, press, d)
    theirs = flux(other, vel_o, press_o, d)
    lam = jnp.maximum(
        jnp.abs(vel[d]) + jnp.sqrt(GAMMA * press * inv),
        jnp.abs(vel_o[d]) + jnp.sqrt(GAMMA * press_o * inv_o),
    )
    return [
        LIFT * (sign * (theirs[v] - mine[v]) + lam * (other[v] - u[v])) for v in range(5)
    ]


def eye_of(rows, width):
    row = lax.broadcasted_iota(jnp.int32, (rows, width), 0)
    col = lax.broadcasted_iota(jnp.int32, (rows, width), 1)
    return row == col


def pack_faces(u_ref, xf_ref, y0_ref, y1_ref, z0_ref, z1_ref):
    nx, ny, nz = u_ref.shape[1:]
    width = z0_ref.shape[2]
    eye = eye_of(ny, width)
    for v in range(5):
        xf_ref[0, v] = u_ref[v, 0]
        xf_ref[1, v] = u_ref[v, nx - 1]
        for x in range(nx):
            y0_ref[v, x : x + 1, :] = u_ref[v, x, 0:1, :]
            y1_ref[v, x : x + 1, :] = u_ref[v, x, ny - 1 : ny, :]
            for ref, at in ((z0_ref, 0), (z1_ref, nz - 1)):
                column = jnp.broadcast_to(u_ref[v, x, :, at : at + 1], (ny, width))
                ref[v, x : x + 1, :] = jnp.sum(
                    jnp.where(eye, column, 0.0), axis=0, keepdims=True
                )


def start_kernel(u_ref, xf_ref, y0_ref, y1_ref, z0_ref, z1_ref, top_ref):
    nx, ny, nz = u_ref.shape[1:]
    pack_faces(u_ref, xf_ref, y0_ref, y1_ref, z0_ref, z1_ref)

    def layer(x, best):
        u = [u_ref[v, x] for v in range(5)]
        inv = 1.0 / u[0]
        mom_sq = u[1] * u[1] + u[2] * u[2] + u[3] * u[3]
        press = GM1 * (u[4] - 0.5 * mom_sq * inv)
        return jnp.maximum(best, jnp.sqrt(mom_sq) * inv + jnp.sqrt(GAMMA * press * inv))

    best = lax.fori_loop(0, nx, layer, jnp.zeros((ny, nz), jnp.float32))
    top_ref[...] = jnp.full(top_ref.shape, jnp.max(best), jnp.float32)


def volume_kernel(
    u_ref, cyh_ref, cyl_ref, czh_ref, czl_ref, mask_ref, r_ref, fy_ref, fz_ref
):
    nx, ny, nz = u_ref.shape[1:]
    tiles = nz // LANES
    diff = -SCALE * gll_derivative()
    half = NODES // 2
    even = [[float(0.5 * (diff[i, j] + diff[i, 5 - j])) for j in range(half)] for i in range(half)]
    odd = [[float(0.5 * (diff[i, j] - diff[i, 5 - j])) for j in range(half)] for i in range(half)]

    def chunk(i, carry):
        row = (i // tiles) * ROWS
        rows = pl.ds(pl.multiple_of(row, ROWS), ROWS)
        cols = pl.ds(pl.multiple_of((i % tiles) * LANES, LANES), LANES)
        for first in range(0, nx, NODES):
            fx = []
            for x in range(first, first + NODES):
                u = [u_ref[v, x, rows, cols] for v in range(5)]
                inv, vel, press = primitives(u)
                fx.append(flux(u, vel, press, 0))
                fy = flux(u, vel, press, 1)
                fz = flux(u, vel, press, 2)
                at = pl.ds(pl.multiple_of(x * ny + row, ROWS), ROWS)
                for v in range(5):
                    fy_ref[v, at, cols] = fy[v]
                    fz_ref[v, at, cols] = fz[v]
            for v in range(5):
                plus = [fx[j][v] + fx[5 - j][v] for j in range(half)]
                minus = [fx[j][v] - fx[5 - j][v] for j in range(half)]
                for k in range(half):
                    a = sum(even[k][j] * plus[j] for j in range(half))
                    b = sum(odd[k][j] * minus[j] for j in range(half))
                    r_ref[v, first + k, rows, cols] = b + a
                    r_ref[v, first + 5 - k, rows, cols] = b - a
        for up in range(NODES, nx, NODES):
            low_u = [u_ref[v, up - 1, rows, cols] for v in range(5)]
            up_u = [u_ref[v, up, rows, cols] for v in range(5)]
            low_lift = face_lift(low_u, up_u, 0, -1.0)
            up_lift = face_lift(up_u, low_u, 0, 1.0)
            for v in range(5):
                r_ref[v, up - 1, rows, cols] += low_lift[v]
                r_ref[v, up, rows, cols] += up_lift[v]
        return carry

    lax.fori_loop(0, (ny // ROWS) * tiles, chunk, 0)

    def layer(x, carry):
        u = [u_ref[v, x] for v in range(5)]
        inv, vel, press = primitives(u)
        sound = jnp.sqrt(GAMMA * press * inv)
        for d, axis, length in ((1, 0, ny), (2, 1, nz)):
            is_last = mask_ref[2 * axis] > 0.5
            weight = mask_ref[2 * axis + 1]

            def outer(a):
                return jnp.where(
                    is_last, pltpu.roll(a, length - 1, axis), pltpu.roll(a, 1, axis)
                )

            speed = jnp.abs(vel[d]) + sound
            lam = weight * jnp.maximum(speed, outer(speed))
            for v in range(5):
                r_ref[v, x] += lam * (outer(u[v]) - u[v])
        return carry

    lax.fori_loop(0, nx, layer, 0)

    def halves(a):
        high = a.astype(jnp.bfloat16)
        return high, (a - high.astype(jnp.float32)).astype(jnp.bfloat16)

    def dot(a, b):
        return jnp.dot(a, b, preferred_element_type=jnp.float32)

    for v in range(5):
        high, low = halves(fz_ref[v])
        acc = dot(high, czl_ref[...]) + dot(low, czh_ref[...]) + dot(high, czh_ref[...])
        high, low = halves(fy_ref[v])
        acc = acc + dot(cyl_ref[...], high) + dot(cyh_ref[...], low) + dot(cyh_ref[...], high)
        r_ref[v] += acc.reshape(nx, ny, nz)


def make_finish(coef_a, coef_b, tops, packs):
    def finish_kernel(*refs):
        top_refs = refs[:tops]
        u_ref, r_ref, reg_ref, xh_ref, yb_ref, ya_ref, zb_ref, za_ref, z0_ref, z1_ref = refs[
            tops : tops + 10
        ]
        new_ref, k_ref = refs[tops + 10 : tops + 12]
        nx, ny, nz = u_ref.shape[1:]
        top = top_refs[0][...]
        for ref in top_refs[1:]:
            top = jnp.maximum(top, ref[...])
        step = jnp.max(COURANT * ELEM_WIDTH / (11.0 * top))

        def advance(x, carry):
            for v in range(5):
                k_ref[v, x] = coef_a * reg_ref[v, x] + step * r_ref[v, x]
            return carry

        lax.fori_loop(0, nx, advance, 0)

        def x_faces(i, carry):
            rows = pl.ds(pl.multiple_of(i * ROWS, ROWS), ROWS)
            for x, side, sign in ((0, 1, 1.0), (nx - 1, 0, -1.0)):
                u = [u_ref[v, x, rows, :] for v in range(5)]
                other = [xh_ref[side, v, rows, :] for v in range(5)]
                lift = face_lift(u, other, 0, sign)
                for v in range(5):
                    k_ref[v, x, rows, :] += step * lift[v]
            return carry

        lax.fori_loop(0, ny // ROWS, x_faces, 0)

        for y, halo, sign in ((0, yb_ref, 1.0), (ny - 1, ya_ref, -1.0)):
            u = [
                jnp.concatenate([u_ref[v, x, y : y + 1, :] for x in range(nx)], axis=0)
                for v in range(5)
            ]
            lift = face_lift(u, [halo[v] for v in range(5)], 1, sign)
            for v in range(5):
                for x in range(nx):
                    k_ref[v, x, y : y + 1, :] += step * lift[v][x : x + 1, :]

        eye = eye_of(ny, z0_ref.shape[2])
        for own, halo, at, sign in ((z0_ref, zb_ref, 0, 1.0), (z1_ref, za_ref, nz - 1, -1.0)):
            lift = face_lift(
                [own[v] for v in range(5)], [halo[v] for v in range(5)], 2, sign
            )
            for v in range(5):
                for x in range(nx):
                    line = jnp.broadcast_to(lift[v][x : x + 1, :], eye.shape)
                    column = jnp.sum(jnp.where(eye, line, 0.0), axis=1, keepdims=True)
                    k_ref[v, x, :, at : at + 1] += step * column

        def update(x, carry):
            for v in range(5):
                new_ref[v, x] = u_ref[v, x] + coef_b * k_ref[v, x]
            return carry

        lax.fori_loop(0, nx, update, 0)
        if packs:
            pack_faces(new_ref, *refs[tops + 12 :])

    return finish_kernel


def swap_faces(faces):
    xf, y0, y1, z0, z1 = faces

    def pair(first, last, axis):
        count = lax.axis_size(axis)
        up = [(i, (i + 1) % count) for i in range(count)]
        down = [(j, i) for i, j in up]
        return lax.ppermute(last, axis, up), lax.ppermute(first, axis, down)

    count = lax.axis_size("gx")
    if count == 2:
        xh = lax.ppermute(xf, "gx", [(0, 1), (1, 0)])
    else:
        before, after = pair(xf[0], xf[1], "gx")
        xh = jnp.stack([after, before])
    yb, ya = pair(y0, y1, "gy")
    zb, za = pair(z0, z1, "gz")
    return xh, yb, ya, zb, za


def others(value, axis):
    count = lax.axis_size(axis)
    return [
        lax.ppermute(value, axis, [(i, (i + s) % count) for i in range(count)])
        for s in range(1, count)
    ]


def shards(state, register):
    nv, nx, ny, nz = state.shape
    width = -(-ny // LANES) * LANES

    def like(*shape):
        return jax.ShapeDtypeStruct(shape, jnp.float32)

    face_shapes = [
        like(2, nv, ny, nz),
        like(nv, nx, nz),
        like(nv, nx, nz),
        like(nv, nx, width),
        like(nv, nx, width),
    ]
    whole = like(*state.shape)
    czh, czl = split_bf16(flux_matrix(nz).T)
    cyh, cyl = split_bf16(np.kron(np.eye(nx), flux_matrix(ny)))
    y_last, y_weight = face_masks(ny)
    z_last, z_weight = face_masks(nz)
    ones = np.ones((ny, nz), np.float32)
    masks = jnp.asarray(
        np.stack([y_last[:, None] * ones, y_weight[:, None] * ones, z_last * ones, z_weight * ones])
    )

    *faces, local_top = pl.pallas_call(
        start_kernel, out_shape=face_shapes + [like(ROWS, LANES)], name="start"
    )(state)

    volume = pl.pallas_call(
        volume_kernel,
        out_shape=whole,
        scratch_shapes=[pltpu.VMEM((nv, nx * ny, nz), jnp.float32)] * 2,
        name="volume",
    )

    def stage(value, axis):
        for other in others(value, axis):
            value = jnp.maximum(value, other)
        return value

    halo = swap_faces(faces)
    top = stage(stage(local_top, "gx"), "gy")
    tops = [top] + others(top, "gz")
    res = volume(state, cyh, cyl, czh, czl, masks)
    first = make_finish(*COEFFS[0], len(tops), True)
    u1, k1, *faces1 = pl.pallas_call(
        first, out_shape=[whole, whole] + face_shapes, name="finish_one"
    )(*tops, state, res, register, *halo, faces[3], faces[4])
    halo1 = swap_faces(faces1)
    res1 = volume(u1, cyh, cyl, czh, czl, masks)
    second = make_finish(*COEFFS[1], len(tops), False)
    new_state, new_register = pl.pallas_call(
        second, out_shape=[whole, whole], name="finish_two"
    )(*tops, u1, res1, k1, *halo1, faces1[3], faces1[4])
    return (new_state, new_register)


def solution(mesh):
    spec = P(None, "gx", "gy", "gz")
    return jax.shard_map(
        shards, mesh=mesh, in_specs=(spec, spec), out_specs=(spec, spec), check_vma=False
    )
```

```python
import math

import jax
import jax.numpy as jnp
import numpy as np
from jax import lax
from jax.experimental import pallas as pl
from jax.experimental.pallas import tpu as pltpu
from jax.sharding import PartitionSpec as P

GAMMA = 1.4
GM1 = 0.4
ELEM_WIDTH = 0.05
COURANT = 0.5
INV_W = 15.0
NODES = 6
SCALE = 2.0 / ELEM_WIDTH
LIFT = 0.5 * SCALE * INV_W
COEFFS = (
    (-567301805773.0 / 1357537059087.0, 5161836677717.0 / 13612068292357.0),
    (-2404267990393.0 / 2016746695238.0, 1720146321549.0 / 2090206949498.0),
)
LANES = 128
ROWS = 8


def gll_derivative():
    seven = math.sqrt(7.0)
    inner = math.sqrt(1.0 / 3.0 - 2.0 * seven / 21.0)
    outer = math.sqrt(1.0 / 3.0 + 2.0 * seven / 21.0)
    points = np.array([-1.0, -outer, -inner, inner, outer, 1.0])
    count = len(points)
    weights = np.array(
        [np.prod([points[i] - points[j] for j in range(count) if j != i]) for i in range(count)]
    )
    table = np.zeros((count, count))
    for i in range(count):
        for j in range(count):
            if i != j:
                table[i, j] = weights[i] / weights[j] / (points[i] - points[j])
        table[i, i] = -np.sum(table[i])
    return table


def flux_matrix(length):
    table = np.kron(np.eye(length // NODES), -SCALE * gll_derivative())
    for up in range(NODES, length, NODES):
        low = up - 1
        table[low, low] += LIFT
        table[low, up] -= LIFT
        table[up, low] += LIFT
        table[up, up] -= LIFT
    return table


def split_bf16(table):
    table = np.asarray(table, np.float32)
    high = table.astype(jnp.bfloat16)
    low = (table - high.astype(np.float32)).astype(jnp.bfloat16)
    return jnp.asarray(high), jnp.asarray(low)


def face_masks(length):
    place = np.arange(length)
    last = (place % NODES == NODES - 1).astype(np.float32)
    ends = (place % NODES == 0) | (place % NODES == NODES - 1)
    ends = ends & (place != 0) & (place != length - 1)
    return last, LIFT * ends.astype(np.float32)


def primitives(u):
    inv = 1.0 / u[0]
    vel = [u[1] * inv, u[2] * inv, u[3] * inv]
    kinetic = u[1] * vel[0] + u[2] * vel[1] + u[3] * vel[2]
    press = GM1 * (u[4] - 0.5 * kinetic)
    return inv, vel, press


def flux(u, vel, press, d):
    v = vel[d]
    parts = [u[1 + d], u[1] * v, u[2] * v, u[3] * v, (u[4] + press) * v]
    parts[1 + d] = parts[1 + d] + press
    return parts


def face_lift(u, other, d, sign):
    inv, vel, press = primitives(u)
    inv_o, vel_o, press_o = primitives(other)
    mine = flux(u, vel, press, d)
    theirs = flux(other, vel_o, press_o, d)
    lam = jnp.maximum(
        jnp.abs(vel[d]) + jnp.sqrt(GAMMA * press * inv),
        jnp.abs(vel_o[d]) + jnp.sqrt(GAMMA * press_o * inv_o),
    )
    return [
        LIFT * (sign * (theirs[v] - mine[v]) + lam * (other[v] - u[v])) for v in range(5)
    ]


def eye_of(rows, width):
    row = lax.broadcasted_iota(jnp.int32, (rows, width), 0)
    col = lax.broadcasted_iota(jnp.int32, (rows, width), 1)
    return row == col


def pack_faces(u_ref, xf_ref, y0_ref, y1_ref, z0_ref, z1_ref):
    nx, ny, nz = u_ref.shape[1:]
    width = z0_ref.shape[2]
    eye = eye_of(ny, width)
    for v in range(5):
        xf_ref[0, v] = u_ref[v, 0]
        xf_ref[1, v] = u_ref[v, nx - 1]
        for x in range(nx):
            y0_ref[v, x : x + 1, :] = u_ref[v, x, 0:1, :]
            y1_ref[v, x : x + 1, :] = u_ref[v, x, ny - 1 : ny, :]
            for ref, at in ((z0_ref, 0), (z1_ref, nz - 1)):
                column = jnp.broadcast_to(u_ref[v, x, :, at : at + 1], (ny, width))
                ref[v, x : x + 1, :] = jnp.sum(
                    jnp.where(eye, column, 0.0), axis=0, keepdims=True
                )


def start_kernel(u_ref, xf_ref, y0_ref, y1_ref, z0_ref, z1_ref, top_ref):
    nx, ny, nz = u_ref.shape[1:]
    pack_faces(u_ref, xf_ref, y0_ref, y1_ref, z0_ref, z1_ref)

    def layer(x, best):
        u = [u_ref[v, x] for v in range(5)]
        inv = 1.0 / u[0]
        mom_sq = u[1] * u[1] + u[2] * u[2] + u[3] * u[3]
        press = GM1 * (u[4] - 0.5 * mom_sq * inv)
        return jnp.maximum(best, jnp.sqrt(mom_sq) * inv + jnp.sqrt(GAMMA * press * inv))

    best = lax.fori_loop(0, nx, layer, jnp.zeros((ny, nz), jnp.float32))
    top_ref[...] = jnp.full(top_ref.shape, jnp.max(best), jnp.float32)


def x_kernel(u_ref, top_ref, r_ref, tick_ref):
    nx, ny, nz = u_ref.shape[1:]
    tick_ref[...] = top_ref[...]
    tiles = nz // LANES
    diff = -SCALE * gll_derivative()
    half = NODES // 2
    even = [[float(0.5 * (diff[i, j] + diff[i, 5 - j])) for j in range(half)] for i in range(half)]
    odd = [[float(0.5 * (diff[i, j] - diff[i, 5 - j])) for j in range(half)] for i in range(half)]

    def chunk(i, carry):
        rows = pl.ds(pl.multiple_of((i // tiles) * ROWS, ROWS), ROWS)
        cols = pl.ds(pl.multiple_of((i % tiles) * LANES, LANES), LANES)
        for first in range(0, nx, NODES):
            fx = []
            for x in range(first, first + NODES):
                u = [u_ref[v, x, rows, cols] for v in range(5)]
                inv, vel, press = primitives(u)
                fx.append(flux(u, vel, press, 0))
            for v in range(5):
                plus = [fx[j][v] + fx[5 - j][v] for j in range(half)]
                minus = [fx[j][v] - fx[5 - j][v] for j in range(half)]
                for k in range(half):
                    a = sum(even[k][j] * plus[j] for j in range(half))
                    b = sum(odd[k][j] * minus[j] for j in range(half))
                    r_ref[v, first + k, rows, cols] = b + a
                    r_ref[v, first + 5 - k, rows, cols] = b - a
        for up in range(NODES, nx, NODES):
            low_u = [u_ref[v, up - 1, rows, cols] for v in range(5)]
            up_u = [u_ref[v, up, rows, cols] for v in range(5)]
            low_lift = face_lift(low_u, up_u, 0, -1.0)
            up_lift = face_lift(up_u, low_u, 0, 1.0)
            for v in range(5):
                r_ref[v, up - 1, rows, cols] += low_lift[v]
                r_ref[v, up, rows, cols] += up_lift[v]
        return carry

    lax.fori_loop(0, (ny // ROWS) * tiles, chunk, 0)


def jump_kernel(u_ref, part_ref, mask_ref, top_ref, r_ref, tick_ref):
    nx, ny, nz = u_ref.shape[1:]
    tick_ref[...] = top_ref[...]

    def layer(x, carry):
        u = [u_ref[v, x] for v in range(5)]
        inv, vel, press = primitives(u)
        sound = jnp.sqrt(GAMMA * press * inv)
        lams = []
        outers = []
        for d, axis, length in ((1, 0, ny), (2, 1, nz)):
            is_last = mask_ref[2 * axis] > 0.5
            weight = mask_ref[2 * axis + 1]

            def outer(a, is_last=is_last, axis=axis, length=length):
                return jnp.where(
                    is_last, pltpu.roll(a, length - 1, axis), pltpu.roll(a, 1, axis)
                )

            speed = jnp.abs(vel[d]) + sound
            lams.append(weight * jnp.maximum(speed, outer(speed)))
            outers.append(outer)
        for v in range(5):
            r_ref[v, x] = (
                part_ref[v, x]
                + lams[0] * (outers[0](u[v]) - u[v])
                + lams[1] * (outers[1](u[v]) - u[v])
            )
        return carry

    lax.fori_loop(0, nx, layer, 0)


def matmul_kernel(
    u_ref, part_ref, cyh_ref, cyl_ref, czh_ref, czl_ref, top_ref, r_ref, tick_ref, fy_ref, fz_ref
):
    nx, ny, nz = u_ref.shape[1:]
    tick_ref[...] = top_ref[...]

    def layer(x, carry):
        u = [u_ref[v, x] for v in range(5)]
        inv, vel, press = primitives(u)
        fy = flux(u, vel, press, 1)
        fz = flux(u, vel, press, 2)
        at = pl.ds(pl.multiple_of(x * ny, ROWS), ny)
        for v in range(5):
            fy_ref[v, at, :] = fy[v]
            fz_ref[v, at, :] = fz[v]
        return carry

    lax.fori_loop(0, nx, layer, 0)

    def halves(a):
        high = a.astype(jnp.bfloat16)
        return high, (a - high.astype(jnp.float32)).astype(jnp.bfloat16)

    def dot(a, b):
        return jnp.dot(a, b, preferred_element_type=jnp.float32)

    for v in range(5):
        high, low = halves(fz_ref[v])
        acc = dot(high, czl_ref[...]) + dot(low, czh_ref[...]) + dot(high, czh_ref[...])
        high, low = halves(fy_ref[v])
        acc = acc + dot(cyl_ref[...], high) + dot(cyh_ref[...], low) + dot(cyh_ref[...], high)
        r_ref[v] = part_ref[v] + acc.reshape(nx, ny, nz)


def make_finish(coef_a, coef_b, tops, last):
    def finish_kernel(*refs):
        top_refs = refs[:tops]
        u_ref, r_ref, reg_ref, xh_ref, yb_ref, ya_ref, zb_ref, za_ref, z0_ref, z1_ref = refs[
            tops : tops + 10
        ]
        out_refs = refs[tops + 10 : tops + 12]
        nx, ny, nz = u_ref.shape[1:]
        if last:
            new_ref, k_ref, sems = refs[tops + 12 :]
        else:
            new_ref, k_ref = out_refs
        top = top_refs[0][...]
        for ref in top_refs[1:]:
            top = jnp.maximum(top, ref[...])
        step = jnp.max(COURANT * ELEM_WIDTH / (11.0 * top))

        y_lifts = []
        for y, halo, sign in ((0, yb_ref, 1.0), (ny - 1, ya_ref, -1.0)):
            u = [
                jnp.concatenate([u_ref[v, x, y : y + 1, :] for x in range(nx)], axis=0)
                for v in range(5)
            ]
            y_lifts.append(face_lift(u, [halo[v] for v in range(5)], 1, sign))
        z_lifts = []
        for own, halo, sign in ((z0_ref, zb_ref, 1.0), (z1_ref, za_ref, -1.0)):
            z_lifts.append(
                face_lift([own[v] for v in range(5)], [halo[v] for v in range(5)], 2, sign)
            )

        eye = eye_of(ny, z0_ref.shape[2])
        row8 = lax.broadcasted_iota(jnp.int32, (ROWS, nz), 0)
        lane = lax.broadcasted_iota(jnp.int32, (ny, LANES), 1)

        def edge(v, x):
            low = jnp.where(row8 == 0, jnp.broadcast_to(y_lifts[0][v][x : x + 1, :], row8.shape), 0.0)
            high = jnp.where(
                row8 == ROWS - 1, jnp.broadcast_to(y_lifts[1][v][x : x + 1, :], row8.shape), 0.0
            )
            middle = [jnp.zeros((ny - 2 * ROWS, nz), jnp.float32)] if ny > 2 * ROWS else []
            rows = jnp.concatenate([low] + middle + [high], axis=0) if ny > ROWS else low + high
            ends = []
            for side, at in ((0, 0), (1, LANES - 1)):
                line = jnp.broadcast_to(z_lifts[side][v][x : x + 1, :], eye.shape)
                column = jnp.sum(jnp.where(eye, line, 0.0), axis=1, keepdims=True)
                ends.append(jnp.where(lane == at, jnp.broadcast_to(column, lane.shape), 0.0))
            inner = [jnp.zeros((ny, nz - 2 * LANES), jnp.float32)] if nz > 2 * LANES else []
            cols = (
                jnp.concatenate([ends[0]] + inner + [ends[1]], axis=1)
                if nz > LANES
                else ends[0] + ends[1]
            )
            return rows + cols

        copies = []
        for x in range(nx):
            lift = [edge(v, x) for v in range(5)]
            for at, side, sign in ((0, 1, 1.0), (nx - 1, 0, -1.0)):
                if x == at:
                    u = [u_ref[v, x] for v in range(5)]
                    more = face_lift(u, [xh_ref[side, v] for v in range(5)], 0, sign)
                    lift = [p + q for p, q in zip(lift, more)]
            for v in range(5):
                k = coef_a * reg_ref[v, x] + step * (r_ref[v, x] + lift[v])
                k_ref[v, x] = k
                new_ref[v, x] = u_ref[v, x] + coef_b * k
            if last:
                for n, (ref, out) in enumerate(zip((new_ref, k_ref), out_refs)):
                    copy = pltpu.make_async_copy(ref.at[:, x], out.at[:, x], sems.at[2 * x + n])
                    copy.start()
                    copies.append(copy)
        for copy in copies:
            copy.wait()
        if not last:
            pack_faces(new_ref, *refs[tops + 12 :])

    return finish_kernel


def swap_faces(faces):
    xf, y0, y1, z0, z1 = faces

    def pair(first, last, axis):
        count = lax.axis_size(axis)
        up = [(i, (i + 1) % count) for i in range(count)]
        down = [(j, i) for i, j in up]
        return lax.ppermute(last, axis, up), lax.ppermute(first, axis, down)

    count = lax.axis_size("gx")
    if count == 2:
        xh = lax.ppermute(xf, "gx", [(0, 1), (1, 0)])
    else:
        before, after = pair(xf[0], xf[1], "gx")
        xh = jnp.stack([after, before])
    yb, ya = pair(y0, y1, "gy")
    zb, za = pair(z0, z1, "gz")
    return xh, yb, ya, zb, za


def others(value, axis):
    count = lax.axis_size(axis)
    return [
        lax.ppermute(value, axis, [(i, (i + s) % count) for i in range(count)])
        for s in range(1, count)
    ]


def shards(state, register):
    nv, nx, ny, nz = state.shape
    width = -(-ny // LANES) * LANES

    def like(*shape):
        return jax.ShapeDtypeStruct(shape, jnp.float32)

    face_shapes = [
        like(2, nv, ny, nz),
        like(nv, nx, nz),
        like(nv, nx, nz),
        like(nv, nx, width),
        like(nv, nx, width),
    ]
    whole = like(*state.shape)
    czh, czl = split_bf16(flux_matrix(nz).T)
    cyh, cyl = split_bf16(np.kron(np.eye(nx), flux_matrix(ny)))
    y_last, y_weight = face_masks(ny)
    z_last, z_weight = face_masks(nz)
    ones = np.ones((ny, nz), np.float32)
    masks = jnp.asarray(
        np.stack([y_last[:, None] * ones, y_weight[:, None] * ones, z_last * ones, z_weight * ones])
    )

    *faces, local_top = pl.pallas_call(
        start_kernel, out_shape=face_shapes + [like(ROWS, LANES)], name="start"
    )(state)

    small = like(ROWS, LANES)
    x_part = pl.pallas_call(x_kernel, out_shape=[whole, small], name="xpart")
    jump_part = pl.pallas_call(
        jump_kernel, out_shape=[whole, small], input_output_aliases={1: 0}, name="jump"
    )
    matmul_part = pl.pallas_call(
        matmul_kernel,
        out_shape=[whole, small],
        input_output_aliases={1: 0},
        scratch_shapes=[pltpu.VMEM((nv, nx * ny, nz), jnp.float32)] * 2,
        name="matmuls",
    )

    def most(value, more):
        for other in more:
            value = jnp.maximum(value, other)
        return value

    halo = swap_faces(faces)
    from_z = others(local_top, "gz")
    res, tick = x_part(state, local_top)
    top = most(tick, from_z)
    from_y = others(top, "gy")
    res, tick = jump_part(state, res, masks, top)
    top = most(tick, from_y)
    from_x = others(top, "gx")
    res, tick = matmul_part(state, res, cyh, cyl, czh, czl, top)
    tops = [tick] + from_x
    first = make_finish(*COEFFS[0], len(tops), False)
    u1, k1, *faces1 = pl.pallas_call(
        first, out_shape=[whole, whole] + face_shapes, name="finish_one"
    )(*tops, state, res, register, *halo, faces[3], faces[4])
    halo1 = swap_faces(faces1)
    res1, unused = x_part(u1, top)
    res1, unused = jump_part(u1, res1, masks, top)
    res1, unused = matmul_part(u1, res1, cyh, cyl, czh, czl, top)
    second = make_finish(*COEFFS[1], len(tops), True)
    anywhere = pl.BlockSpec(memory_space=pl.ANY)
    new_state, new_register = pl.pallas_call(
        second,
        out_shape=[whole, whole],
        out_specs=[anywhere, anywhere],
        scratch_shapes=[pltpu.VMEM(state.shape, jnp.float32)] * 2
        + [pltpu.SemaphoreType.DMA((2 * nx,))],
        name="finish_two",
    )(*tops, u1, res1, k1, *halo1, faces1[3], faces1[4])
    return (new_state, new_register)


def solution(mesh):
    spec = P(None, "gx", "gy", "gz")
    return jax.shard_map(
        shards, mesh=mesh, in_specs=(spec, spec), out_specs=(spec, spec), check_vma=False
    )
```

```python
import math

import jax
import jax.numpy as jnp
import numpy as np
from jax import lax
from jax.experimental import pallas as pl
from jax.experimental.pallas import tpu as pltpu
from jax.sharding import PartitionSpec as P

GAMMA = 1.4
GM1 = 0.4
ELEM_WIDTH = 0.05
COURANT = 0.5
INV_W = 15.0
NODES = 6
SCALE = 2.0 / ELEM_WIDTH
LIFT = 0.5 * SCALE * INV_W
COEFFS = (
    (-567301805773.0 / 1357537059087.0, 5161836677717.0 / 13612068292357.0),
    (-2404267990393.0 / 2016746695238.0, 1720146321549.0 / 2090206949498.0),
)
LANES = 128
VMEM_LIMIT = 24 * 1024 * 1024
ROWS = 8


def gll_derivative():
    seven = math.sqrt(7.0)
    inner = math.sqrt(1.0 / 3.0 - 2.0 * seven / 21.0)
    outer = math.sqrt(1.0 / 3.0 + 2.0 * seven / 21.0)
    points = np.array([-1.0, -outer, -inner, inner, outer, 1.0])
    count = len(points)
    weights = np.array(
        [np.prod([points[i] - points[j] for j in range(count) if j != i]) for i in range(count)]
    )
    table = np.zeros((count, count))
    for i in range(count):
        for j in range(count):
            if i != j:
                table[i, j] = weights[i] / weights[j] / (points[i] - points[j])
        table[i, i] = -np.sum(table[i])
    return table


def flux_matrix(length):
    table = np.kron(np.eye(length // NODES), -SCALE * gll_derivative())
    for up in range(NODES, length, NODES):
        low = up - 1
        table[low, low] += LIFT
        table[low, up] -= LIFT
        table[up, low] += LIFT
        table[up, up] -= LIFT
    return table


def split_bf16(table):
    table = np.asarray(table, np.float32)
    high = table.astype(jnp.bfloat16)
    low = (table - high.astype(np.float32)).astype(jnp.bfloat16)
    return jnp.asarray(high), jnp.asarray(low)


def face_masks(length):
    place = np.arange(length)
    last = (place % NODES == NODES - 1).astype(np.float32)
    ends = (place % NODES == 0) | (place % NODES == NODES - 1)
    ends = ends & (place != 0) & (place != length - 1)
    return last, LIFT * ends.astype(np.float32)


def primitives(u):
    inv = 1.0 / u[0]
    vel = [u[1] * inv, u[2] * inv, u[3] * inv]
    kinetic = u[1] * vel[0] + u[2] * vel[1] + u[3] * vel[2]
    press = GM1 * (u[4] - 0.5 * kinetic)
    return inv, vel, press


def flux(u, vel, press, d):
    v = vel[d]
    parts = [u[1 + d], u[1] * v, u[2] * v, u[3] * v, (u[4] + press) * v]
    parts[1 + d] = parts[1 + d] + press
    return parts


def face_lift(u, other, d, sign):
    inv, vel, press = primitives(u)
    inv_o, vel_o, press_o = primitives(other)
    mine = flux(u, vel, press, d)
    theirs = flux(other, vel_o, press_o, d)
    lam = jnp.maximum(
        jnp.abs(vel[d]) + jnp.sqrt(GAMMA * press * inv),
        jnp.abs(vel_o[d]) + jnp.sqrt(GAMMA * press_o * inv_o),
    )
    return [
        LIFT * (sign * (theirs[v] - mine[v]) + lam * (other[v] - u[v])) for v in range(5)
    ]


def eye_of(rows, width):
    row = lax.broadcasted_iota(jnp.int32, (rows, width), 0)
    col = lax.broadcasted_iota(jnp.int32, (rows, width), 1)
    return row == col


def pack_faces(u_ref, xf_ref, y0_ref, y1_ref, z0_ref, z1_ref):
    nx, ny, nz = u_ref.shape[1:]
    width = z0_ref.shape[2]
    eye = eye_of(ny, width)
    for v in range(5):
        xf_ref[0, v] = u_ref[v, 0]
        xf_ref[1, v] = u_ref[v, nx - 1]
        for x in range(nx):
            y0_ref[v, x : x + 1, :] = u_ref[v, x, 0:1, :]
            y1_ref[v, x : x + 1, :] = u_ref[v, x, ny - 1 : ny, :]
            for ref, at in ((z0_ref, 0), (z1_ref, nz - 1)):
                column = jnp.broadcast_to(u_ref[v, x, :, at : at + 1], (ny, width))
                ref[v, x : x + 1, :] = jnp.sum(
                    jnp.where(eye, column, 0.0), axis=0, keepdims=True
                )


def pack_kernel(u_ref, top_ref, xf_ref, y0_ref, y1_ref, z0_ref, z1_ref, tick_ref):
    tick_ref[...] = top_ref[...]
    pack_faces(u_ref, xf_ref, y0_ref, y1_ref, z0_ref, z1_ref)


def top_kernel(u_ref, top_ref):
    nx, ny, nz = u_ref.shape[1:]

    def layer(x, best):
        u = [u_ref[v, x] for v in range(5)]
        inv = 1.0 / u[0]
        mom_sq = u[1] * u[1] + u[2] * u[2] + u[3] * u[3]
        press = GM1 * (u[4] - 0.5 * mom_sq * inv)
        return jnp.maximum(best, jnp.sqrt(mom_sq) * inv + jnp.sqrt(GAMMA * press * inv))

    best = lax.fori_loop(0, nx, layer, jnp.zeros((ny, nz), jnp.float32))
    top_ref[...] = jnp.full(top_ref.shape, jnp.max(best), jnp.float32)


def volume_kernel(
    u_ref, cyh_ref, cyl_ref, czh_ref, czl_ref, mask_ref, top_ref, r_ref, tick_ref, fy_ref, fz_ref
):
    nx, ny, nz = u_ref.shape[1:]
    tick_ref[...] = top_ref[...]
    tiles = nz // LANES
    diff = -SCALE * gll_derivative()
    half = NODES // 2
    even = [[float(0.5 * (diff[i, j] + diff[i, 5 - j])) for j in range(half)] for i in range(half)]
    odd = [[float(0.5 * (diff[i, j] - diff[i, 5 - j])) for j in range(half)] for i in range(half)]

    def chunk(i, carry):
        row = (i // tiles) * ROWS
        rows = pl.ds(pl.multiple_of(row, ROWS), ROWS)
        cols = pl.ds(pl.multiple_of((i % tiles) * LANES, LANES), LANES)
        for first in range(0, nx, NODES):
            fx = []
            for x in range(first, first + NODES):
                u = [u_ref[v, x, rows, cols] for v in range(5)]
                inv, vel, press = primitives(u)
                fx.append(flux(u, vel, press, 0))
                fy = flux(u, vel, press, 1)
                fz = flux(u, vel, press, 2)
                at = pl.ds(pl.multiple_of(x * ny + row, ROWS), ROWS)
                for v in range(5):
                    fy_ref[v, at, cols] = fy[v]
                    fz_ref[v, at, cols] = fz[v]
            for v in range(5):
                plus = [fx[j][v] + fx[5 - j][v] for j in range(half)]
                minus = [fx[j][v] - fx[5 - j][v] for j in range(half)]
                for k in range(half):
                    a = sum(even[k][j] * plus[j] for j in range(half))
                    b = sum(odd[k][j] * minus[j] for j in range(half))
                    r_ref[v, first + k, rows, cols] = b + a
                    r_ref[v, first + 5 - k, rows, cols] = b - a
        for up in range(NODES, nx, NODES):
            low_u = [u_ref[v, up - 1, rows, cols] for v in range(5)]
            up_u = [u_ref[v, up, rows, cols] for v in range(5)]
            low_lift = face_lift(low_u, up_u, 0, -1.0)
            up_lift = face_lift(up_u, low_u, 0, 1.0)
            for v in range(5):
                r_ref[v, up - 1, rows, cols] += low_lift[v]
                r_ref[v, up, rows, cols] += up_lift[v]
        return carry

    lax.fori_loop(0, (ny // ROWS) * tiles, chunk, 0)

    def layer(x, carry):
        u = [u_ref[v, x] for v in range(5)]
        inv, vel, press = primitives(u)
        sound = jnp.sqrt(GAMMA * press * inv)
        for d, axis, length in ((1, 0, ny), (2, 1, nz)):
            is_last = mask_ref[2 * axis] > 0.5
            weight = mask_ref[2 * axis + 1]

            def outer(a):
                return jnp.where(
                    is_last, pltpu.roll(a, length - 1, axis), pltpu.roll(a, 1, axis)
                )

            speed = jnp.abs(vel[d]) + sound
            lam = weight * jnp.maximum(speed, outer(speed))
            for v in range(5):
                r_ref[v, x] += lam * (outer(u[v]) - u[v])
        return carry

    lax.fori_loop(0, nx, layer, 0)

    def halves(a):
        high = a.astype(jnp.bfloat16)
        return high, (a - high.astype(jnp.float32)).astype(jnp.bfloat16)

    def dot(a, b):
        return jnp.dot(a, b, preferred_element_type=jnp.float32)

    for v in range(5):
        high, low = halves(fz_ref[v])
        acc = dot(high, czl_ref[...]) + dot(low, czh_ref[...]) + dot(high, czh_ref[...])
        high, low = halves(fy_ref[v])
        acc = acc + dot(cyl_ref[...], high) + dot(cyh_ref[...], low) + dot(cyh_ref[...], high)
        r_ref[v] += acc.reshape(nx, ny, nz)


def make_finish(coef_a, coef_b, tops, last):
    def finish_kernel(*refs):
        top_refs = refs[:tops]
        u_ref, r_ref, reg_ref, xh_ref, yb_ref, ya_ref, zb_ref, za_ref, z0_ref, z1_ref = refs[
            tops : tops + 10
        ]
        out_refs = refs[tops + 10 : tops + 12]
        nx, ny, nz = u_ref.shape[1:]
        if last:
            new_ref, k_ref, sems = refs[tops + 12 :]
        else:
            new_ref, k_ref = out_refs
        top = top_refs[0][...]
        for ref in top_refs[1:]:
            top = jnp.maximum(top, ref[...])
        step = jnp.max(COURANT * ELEM_WIDTH / (11.0 * top))

        y_lifts = []
        for y, halo, sign in ((0, yb_ref, 1.0), (ny - 1, ya_ref, -1.0)):
            u = [
                jnp.concatenate([u_ref[v, x, y : y + 1, :] for x in range(nx)], axis=0)
                for v in range(5)
            ]
            y_lifts.append(face_lift(u, [halo[v] for v in range(5)], 1, sign))
        z_lifts = []
        for own, halo, sign in ((z0_ref, zb_ref, 1.0), (z1_ref, za_ref, -1.0)):
            z_lifts.append(
                face_lift([own[v] for v in range(5)], [halo[v] for v in range(5)], 2, sign)
            )

        eye = eye_of(ny, z0_ref.shape[2])
        row8 = lax.broadcasted_iota(jnp.int32, (ROWS, nz), 0)
        lane = lax.broadcasted_iota(jnp.int32, (ny, LANES), 1)

        def edge(v, x):
            low = jnp.where(row8 == 0, jnp.broadcast_to(y_lifts[0][v][x : x + 1, :], row8.shape), 0.0)
            high = jnp.where(
                row8 == ROWS - 1, jnp.broadcast_to(y_lifts[1][v][x : x + 1, :], row8.shape), 0.0
            )
            middle = [jnp.zeros((ny - 2 * ROWS, nz), jnp.float32)] if ny > 2 * ROWS else []
            rows = jnp.concatenate([low] + middle + [high], axis=0) if ny > ROWS else low + high
            ends = []
            for side, at in ((0, 0), (1, LANES - 1)):
                line = jnp.broadcast_to(z_lifts[side][v][x : x + 1, :], eye.shape)
                column = jnp.sum(jnp.where(eye, line, 0.0), axis=1, keepdims=True)
                ends.append(jnp.where(lane == at, jnp.broadcast_to(column, lane.shape), 0.0))
            inner = [jnp.zeros((ny, nz - 2 * LANES), jnp.float32)] if nz > 2 * LANES else []
            cols = (
                jnp.concatenate([ends[0]] + inner + [ends[1]], axis=1)
                if nz > LANES
                else ends[0] + ends[1]
            )
            return rows + cols

        copies = []
        for x in range(nx):
            lift = [edge(v, x) for v in range(5)]
            for at, side, sign in ((0, 1, 1.0), (nx - 1, 0, -1.0)):
                if x == at:
                    u = [u_ref[v, x] for v in range(5)]
                    more = face_lift(u, [xh_ref[side, v] for v in range(5)], 0, sign)
                    lift = [p + q for p, q in zip(lift, more)]
            for v in range(5):
                k = coef_a * reg_ref[v, x] + step * (r_ref[v, x] + lift[v])
                k_ref[v, x] = k
                new_ref[v, x] = u_ref[v, x] + coef_b * k
            if last:
                for n, (ref, out) in enumerate(zip((new_ref, k_ref), out_refs)):
                    copy = pltpu.make_async_copy(ref.at[:, x], out.at[:, x], sems.at[2 * x + n])
                    copy.start()
                    copies.append(copy)
        for copy in copies:
            copy.wait()
        if not last:
            pack_faces(new_ref, *refs[tops + 12 :])

    return finish_kernel


def swap_faces(faces):
    xf, y0, y1, z0, z1 = faces

    def pair(first, last, axis):
        count = lax.axis_size(axis)
        up = [(i, (i + 1) % count) for i in range(count)]
        down = [(j, i) for i, j in up]
        return lax.ppermute(last, axis, up), lax.ppermute(first, axis, down)

    count = lax.axis_size("gx")
    if count == 2:
        xh = lax.ppermute(xf, "gx", [(0, 1), (1, 0)])
    else:
        before, after = pair(xf[0], xf[1], "gx")
        xh = jnp.stack([after, before])
    yb, ya = pair(y0, y1, "gy")
    zb, za = pair(z0, z1, "gz")
    return xh, yb, ya, zb, za


def others(value, axis):
    count = lax.axis_size(axis)
    return [
        lax.ppermute(value, axis, [(i, (i + s) % count) for i in range(count)])
        for s in range(1, count)
    ]


def shards(state, register):
    nv, nx, ny, nz = state.shape
    width = -(-ny // LANES) * LANES

    def like(*shape):
        return jax.ShapeDtypeStruct(shape, jnp.float32)

    face_shapes = [
        like(2, nv, ny, nz),
        like(nv, nx, nz),
        like(nv, nx, nz),
        like(nv, nx, width),
        like(nv, nx, width),
    ]
    whole = like(*state.shape)
    czh, czl = split_bf16(flux_matrix(nz).T)
    cyh, cyl = split_bf16(np.kron(np.eye(nx), flux_matrix(ny)))
    y_last, y_weight = face_masks(ny)
    z_last, z_weight = face_masks(nz)
    ones = np.ones((ny, nz), np.float32)
    masks = jnp.asarray(
        np.stack([y_last[:, None] * ones, y_weight[:, None] * ones, z_last * ones, z_weight * ones])
    )

    small = like(ROWS, LANES)
    limits = pltpu.CompilerParams(vmem_limit_bytes=VMEM_LIMIT)
    volume = pl.pallas_call(
        volume_kernel,
        out_shape=[whole, small],
        scratch_shapes=[pltpu.VMEM((nv, nx * ny, nz), jnp.float32)] * 2,
        compiler_params=limits,
        name="volume",
    )

    def most(value, more):
        for other in more:
            value = jnp.maximum(value, other)
        return value

    local_top = pl.pallas_call(
        top_kernel, out_shape=small, compiler_params=limits, name="top"
    )(state)
    from_z = others(local_top, "gz")
    *faces, tick = pl.pallas_call(
        pack_kernel, out_shape=face_shapes + [small], compiler_params=limits, name="pack"
    )(state, local_top)
    halo = swap_faces(faces)
    top = most(tick, from_z)
    top = most(top, others(top, "gy"))
    from_x = others(top, "gx")
    res, tick = volume(state, cyh, cyl, czh, czl, masks, top)
    tops = [tick] + from_x
    first = make_finish(*COEFFS[0], len(tops), False)
    u1, k1, *faces1 = pl.pallas_call(
        first, out_shape=[whole, whole] + face_shapes, compiler_params=limits, name="finish_one"
    )(*tops, state, res, register, *halo, faces[3], faces[4])
    halo1 = swap_faces(faces1)
    res1, unused = volume(u1, cyh, cyl, czh, czl, masks, top)
    second = make_finish(*COEFFS[1], len(tops), True)
    anywhere = pl.BlockSpec(memory_space=pl.ANY)
    new_state, new_register = pl.pallas_call(
        second,
        out_shape=[whole, whole],
        out_specs=[anywhere, anywhere],
        scratch_shapes=[pltpu.VMEM(state.shape, jnp.float32)] * 2
        + [pltpu.SemaphoreType.DMA((2 * nx,))],
        compiler_params=limits,
        name="finish_two",
    )(*tops, u1, res1, k1, *halo1, faces1[3], faces1[4])
    return (new_state, new_register)


def solution(mesh):
    spec = P(None, "gx", "gy", "gz")
    return jax.shard_map(
        shards, mesh=mesh, in_specs=(spec, spec), out_specs=(spec, spec), check_vma=False
    )
```
